32 devices in a mesh: seq: 8 (over z, y), head: 4 (over x, core).
Axes of the slice: x: 2, y: 2, z: 4, core: 2. Of those that a mesh axis runs over, the one named last changes fastest.
Arguments:
- tokens: bfloat16 [6144, 2560], P(('seq', 'head')), may hold values from -12 to 12
- pre_gain: float32 [2560], replicated, may hold values from 0.25 to 1.75
- inner_proj: bfloat16 [2560, 2, 5120], P(None, None, 'head'), may hold values from -0.125 to 0.125
- outer_proj: bfloat16 [2560, 336], replicated, may hold values from -0.125 to 0.125
- kernel_x: float32 [4, 5120], P(None, 'head'), may hold values from -3 to 3
- kernel_bc: float32 [4, 256], replicated, may hold values from -3 to 3
- offset_x: float32 [5120], P('head'), may hold values from -3 to 3
- offset_bc: float32 [256], replicated, may hold values from -3 to 3
- dt_bias: float32 [80], P('head'), may hold values from -7 to -5
- a_log: float32 [80], P('head'), may hold values from -12 to 4
- skip_gain: float32 [80], P('head'), may hold values from 0.5 to 1.5
- norm_gain: float32 [5120], P('head'), may hold values from 0.25 to 1.75
- out_proj: bfloat16 [5120, 2560], P('head'), may hold values from -0.078125 to 0.078125
Outputs:
- mixed: bfloat16 [6144, 2560], P(('seq', 'head'))
The draws below stay inside these ranges and needn't reach their ends.
All inputs are finite; a program needn't handle non-finite values.
Results may differ from the reference program's by a relative error of at most 0.014.
Values may be sent and summed in bfloat16 or wider, within the bound.
No kernel may reach another device: no remote copies, remote signals or barrier semaphores. Data moves between devices by JAX's collectives and lax.ppermute only.
A program may use at most 128 MiB of HBM per device.

```python
import jax
import jax.numpy as jnp
from jax import lax

D = 2560
H = 80
P_SIZE = 64
N = 128
CONV = 4
SPAN = 256
DI = 5120
TOKENS = 6144
N_HEAD = 4


def draw_tokens(key, part):
    noise_key, level_key, course_key = jax.random.split(key, 3)
    blocks = TOKENS // SPAN
    noise = jax.random.normal(noise_key, (TOKENS, D), jnp.float32)
    levels = 2.0 * jax.random.normal(level_key, (blocks, 1, 1), jnp.float32)
    course = jax.random.normal(course_key, (1, 1, D), jnp.float32)
    shifted = noise.reshape(blocks, SPAN, D) + levels * course
    return jnp.clip(shifted.reshape(TOKENS, D), -12.0, 12.0).astype(jnp.bfloat16)


def draw_a_log(key, part):
    order_key, rate_key = jax.random.split(key)
    order = jax.random.permutation(order_key, H)
    share = H // 2
    quick = order < share
    spread = jax.random.uniform(rate_key, (H,), jnp.float32)
    quick_rate = jnp.log(4.0) + spread * jnp.log(10.0)
    patient_rate = jnp.log(10.0 / TOKENS) + spread * jnp.log(10.0)
    return jnp.where(quick, quick_rate, patient_rate).astype(jnp.float32)


def block_levels(own_key, dims, cuts, least, top_value):
    level = 1.0
    for dim, blocks in cuts:
        heights = jax.random.uniform(jax.random.fold_in(jax.random.fold_in(own_key, 6), dim), (blocks,), jnp.float32, least / len(cuts), top_value / len(cuts))
        level = level * jnp.repeat(jnp.exp(heights), dims[dim] // blocks).reshape((-1,) + (1,) * (len(dims) - 1 - dim))
    return level


def normal_values(stream_key, dims, scale, limit, cuts=(), kind=jnp.bfloat16):
    drawn = jax.random.normal(stream_key, dims, jnp.float32) * scale
    if len(cuts) > 0:
        drawn = block_levels(stream_key, dims, cuts, -0.22, 0.18) * drawn
    return jnp.clip(drawn, min=-limit, max=limit).astype(kind)


def setup_inputs(seed: int = 0) -> dict:
    streams_of = jax.random.split(jax.random.key(seed), 14)
    tokens = draw_tokens(jax.random.fold_in(streams_of[13], 71), 0)
    pre_gain = jnp.clip(1.0 + 0.15 * jax.random.normal(streams_of[1], (D,), jnp.float32), 0.25, 1.75)
    inner_proj = normal_values(streams_of[2], (D, 2, DI), D ** -0.5, 0.125, ((2, 4),))
    outer_proj = normal_values(streams_of[3], (D, 2 * N + H), D ** -0.5, 0.125)
    kernel_x = normal_values(streams_of[4], (CONV, DI), CONV ** -0.5, 3.0, ((1, 4),), jnp.float32)
    kernel_bc = normal_values(streams_of[5], (CONV, 2 * N), CONV ** -0.5, 3.0, (), jnp.float32)
    offset_x = normal_values(streams_of[6], (DI,), 0.5, 3.0, ((0, 4),), jnp.float32)
    offset_bc = normal_values(streams_of[7], (2 * N,), 0.5, 3.0, (), jnp.float32)
    dt_bias = jnp.clip(-7.0 + 2.0 * jax.random.uniform(streams_of[8], (H,), jnp.float32) ** block_levels(streams_of[8], (H,), ((0, 4),), -0.2, 0.2), -7.0, -5.0)
    a_log = draw_a_log(jax.random.fold_in(streams_of[13], 71), 0)
    skip_gain = jnp.clip(0.5 + 1.0 * jax.random.uniform(streams_of[10], (H,), jnp.float32) ** block_levels(streams_of[10], (H,), ((0, 4),), -0.2, 0.2), 0.5, 1.5)
    norm_gain = jnp.clip(1.0 + 0.15 * jax.random.normal(streams_of[11], (DI,), jnp.float32), 0.25, 1.75)
    out_proj = normal_values(streams_of[12], (DI, D), DI ** -0.5, 0.078125, ((0, 4),))
    return {"tokens": tokens, "pre_gain": pre_gain, "inner_proj": inner_proj, "outer_proj": outer_proj, "kernel_x": kernel_x, "kernel_bc": kernel_bc, "offset_x": offset_x, "offset_bc": offset_bc, "dt_bias": dt_bias, "a_log": a_log, "skip_gain": skip_gain, "norm_gain": norm_gain, "out_proj": out_proj}


norm_floor = 0.1

def row_norm(row_block, gain_vector):
    widened = row_block.astype(jnp.float32)
    inverse_rms = lax.rsqrt(lax.optimization_barrier(jnp.mean(widened * widened, axis=-1, keepdims=True)) + norm_floor)
    return widened * inverse_rms * gain_vector

def masked_exp(log_gap, causal):
    return jnp.where(causal, jnp.exp(jnp.where(causal, log_gap, 0.0)), 0.0)

def block_scan(values_x, values_b, values_c, step_sizes, decay_rate, ssm_state):
    running = jnp.cumsum(step_sizes * decay_rate, axis=0)
    score_rows = jnp.dot(values_c, values_b.T, preferred_element_type=jnp.float32)
    running_heads = running.T
    row_index = lax.broadcasted_iota(jnp.int32, (SPAN, SPAN), 0)
    col_index = lax.broadcasted_iota(jnp.int32, (SPAN, SPAN), 1)
    decay_factor = masked_exp(running_heads[:, :, None] - running_heads[:, None, :], row_index >= col_index)
    mix_weights = (score_rows[None] * decay_factor * step_sizes.T[:, None, :]).astype(jnp.bfloat16)
    intra_out = jnp.einsum('hts,shp->thp', mix_weights.astype(jnp.float32), values_x.astype(jnp.float32))
    end_weight = jnp.exp(running[-1:] - running) * step_sizes
    scaled_x = (values_x.astype(jnp.float32) * end_weight[:, :, None]).astype(jnp.bfloat16)
    block_state = jnp.einsum('shp,sn->hpn', scaled_x.astype(jnp.float32), values_b.astype(jnp.float32))
    cross_out = jnp.exp(running)[:, :, None] * jnp.einsum('tn,hpn->thp', values_c.astype(jnp.float32), ssm_state, precision=lax.Precision.HIGHEST)
    next_state = jnp.exp(running[-1])[:, None, None] * ssm_state + block_state
    return (intra_out + cross_out, next_state)

def reference(tokens, pre_gain, inner_proj, outer_proj, kernel_x, kernel_bc, offset_x, offset_bc, dt_bias, a_log, skip_gain, norm_gain, out_proj):
    decay_rate = -jnp.exp(a_log)
    joined_proj = inner_proj.reshape(D, 2 * DI)
    conv_weight = jnp.concatenate([kernel_x, kernel_bc], axis=1)
    conv_bias = jnp.concatenate([offset_x, offset_bc])
    group_width = DI // N_HEAD

    def advance(carry, row_block):
        ssm_state, conv_tail = carry
        normed = row_norm(row_block, pre_gain).astype(jnp.bfloat16)
        inner_part = jnp.dot(normed, joined_proj, preferred_element_type=jnp.float32)
        outer_part = jnp.dot(normed, outer_proj, preferred_element_type=jnp.float32)
        gate_in = inner_part[:, :DI].astype(jnp.bfloat16)
        x_in = inner_part[:, DI:].astype(jnp.bfloat16)
        bc_in = outer_part[:, :2 * N].astype(jnp.bfloat16)
        dt_raw = outer_part[:, 2 * N:]
        conv_input = jnp.concatenate([x_in, bc_in], axis=1)
        extended = jnp.concatenate([conv_tail, conv_input], axis=0)
        summed = jnp.broadcast_to(conv_bias, conv_input.shape).astype(jnp.float32)
        for offset in range(CONV):
            summed = summed + conv_weight[offset] * extended[offset:offset + SPAN].astype(jnp.float32)
        conv_out = jax.nn.silu(summed).astype(jnp.bfloat16)
        values_x = conv_out[:, :DI].reshape(SPAN, H, P_SIZE)
        values_b = conv_out[:, DI:DI + N]
        values_c = conv_out[:, DI + N:]
        step_sizes = jax.nn.softplus(dt_raw + dt_bias)
        scan_out, next_state = block_scan(values_x, values_b, values_c, step_sizes, decay_rate, ssm_state)
        mixer_out = (scan_out + skip_gain[:, None] * values_x.astype(jnp.float32)).reshape(SPAN, DI)
        gated = mixer_out * jax.nn.silu(gate_in.astype(jnp.float32))
        normed_out = row_norm(gated, norm_gain).astype(jnp.bfloat16)
        total = jnp.zeros((SPAN, D), jnp.float32)
        for offset in range(N_HEAD):
            lower = offset * group_width
            partial_value = jnp.dot(normed_out[:, lower:lower + group_width], out_proj[lower:lower + group_width], preferred_element_type=jnp.float32).astype(jnp.bfloat16)
            total = total + lax.optimization_barrier(partial_value).astype(jnp.float32)
        next_tail = extended[SPAN:]
        return ((next_state, next_tail), total.astype(jnp.bfloat16))
    start_state = jnp.zeros((H, P_SIZE, N), jnp.float32)
    start_tail = jnp.zeros((CONV - 1, DI + 2 * N), jnp.bfloat16)
    blocks_in = tokens.reshape(TOKENS // SPAN, SPAN, D)
    final_carry, outputs = lax.scan(advance, (start_state, start_tail), blocks_in)
    return outputs.reshape(TOKENS, D)
```

```python
import jax
import jax.numpy as jnp
from jax import lax
from jax.experimental import pallas as pl
from jax.experimental.pallas import tpu as pltpu
from jax.sharding import PartitionSpec as P

SPAN = 256
LANES = 128
HALO = 16

norm_floor = 0.1
bf16 = jnp.bfloat16
f32 = jnp.float32


def swapped(block, axis, distance):
    return lax.ppermute(block, axis, [(i, i ^ distance) for i in range(lax.axis_size(axis))])


def row_norm(row_block, gain_vector):
    widened = row_block.astype(f32)
    inverse_rms = lax.rsqrt(jnp.mean(widened * widened, axis=-1, keepdims=True) + norm_floor)
    return widened * inverse_rms * gain_vector


def half_silu(u):
    v = 0.5 * u
    return v + v * jnp.tanh(v)


def spread(per_head, tile, head_size, lane):
    per_tile = LANES // head_size
    first = tile * per_tile
    out = per_head[:, first : first + 1]
    for k in range(1, per_tile):
        out = jnp.where(lane >= k * head_size, per_head[:, first + k : first + k + 1], out)
    return out


def conv_tile(now, before, taps, bias):
    rows = now.shape[0]
    stacked = jnp.concatenate([before.astype(f32)[HALO - 8 :], now.astype(f32)], axis=0)
    count = taps.shape[0]
    total = bias + taps[count - 1 : count] * stacked[8:]
    for k in range(count - 1):
        moved = pltpu.roll(stacked, count - 1 - k, 0)[8:]
        total = total + taps[k : k + 1] * moved
    return half_silu(total).astype(bf16)


def state_kernel(head_size, x_ref, bc_ref, tail_x_ref, tail_bc_ref, dt_ref, rate_ref, kx_ref, kbc_ref, ox_ref, obc_ref,
                 xc_ref, bco_ref, cum_ref, cumt_ref, dtt_ref, ls_ref, pdec_ref, sum_ref, dec_ref,
                 px, pbc, state, logs, xw):
    step = pl.program_id(0)
    span, width = x_ref.shape
    n = bc_ref.shape[1] // 2

    @pl.when(step == 0)
    def _():
        px[...] = tail_x_ref[...]
        pbc[...] = tail_bc_ref[...]
        state[...] = jnp.zeros_like(state)
        logs[...] = jnp.zeros_like(logs)

    for j in range(2 * n // LANES):
        at = slice(j * LANES, (j + 1) * LANES)
        bco_ref[:, at] = conv_tile(bc_ref[:, at], pbc[:, at], kbc_ref[:, at], obc_ref[:, at])
    row = lax.broadcasted_iota(jnp.int32, (span, span), 0)
    col = lax.broadcasted_iota(jnp.int32, (span, span), 1)
    lower = (row >= col).astype(f32)
    dt = dt_ref[...]
    cum = jnp.dot(lower, dt * rate_ref[...], precision=lax.Precision.HIGHEST, preferred_element_type=f32)
    cum_ref[...] = cum
    cumt_ref[0] = cum.T
    dtt_ref[0] = dt.T
    end = cum[span - 1 :]
    weight = jnp.exp(end - cum) * dt
    ls_ref[0] = state[...]
    pdec_ref[0] = jnp.exp(logs[...])
    lane = lax.broadcasted_iota(jnp.int32, (1, LANES), 1)
    for j in range(width // LANES):
        at = slice(j * LANES, (j + 1) * LANES)
        xb = conv_tile(x_ref[:, at], px[:, at], kx_ref[:, at], ox_ref[:, at])
        xc_ref[:, at] = xb
        xw[:, at] = (xb.astype(f32) * spread(weight, j, head_size, lane)).astype(bf16)
        end_tile = spread(end, j, head_size, lane)
        logs[:, at] = logs[:, at] + end_tile
        state[:, at] = state[:, at] * jnp.exp(end_tile)
    state[...] = state[...] + lax.dot_general(
        bco_ref[:, :n], xw[...], (((0,), (0,)), ((), ())), preferred_element_type=f32
    )
    px[...] = x_ref[span - HALO :, :]
    pbc[...] = bc_ref[span - HALO :, :]

    @pl.when(step == pl.num_programs(0) - 1)
    def _():
        sum_ref[...] = state[...].astype(bf16)
        total = jnp.exp(logs[...])
        high = total.astype(bf16).astype(f32)
        which = lax.broadcasted_iota(jnp.int32, total.shape, 0)
        dec_ref[...] = jnp.where(which == 0, high, jnp.where(which == 1, total - high, 0.0)).astype(bf16)


def inside_kernel(head_size, x_ref, bc_ref, cum_ref, cumt_ref, dtt_ref, skip_ref, y_ref):
    span, width = x_ref.shape
    n = bc_ref.shape[1] // 2
    half = span // 2
    score = lax.dot_general(
        bc_ref[:, n:], bc_ref[:, :n], (((1,), (1,)), ((), ())), preferred_element_type=f32
    )
    row = lax.broadcasted_iota(jnp.int32, (span, span), 0)
    col = lax.broadcasted_iota(jnp.int32, (span, span), 1)
    score = jnp.where(row >= col, score, 0.0)
    top = score[:half, :half]
    low = score[half:]
    per_tile = LANES // head_size
    lane = lax.broadcasted_iota(jnp.int32, (1, LANES), 1)
    for j in range(width // LANES):
        at = slice(j * LANES, (j + 1) * LANES)
        xt = x_ref[:, at]
        up = down = None
        for k in range(per_tile):
            h = j * per_tile + k
            later = cum_ref[:, h : h + 1]
            earlier = cumt_ref[0, h : h + 1, :]
            dt = dtt_ref[0, h : h + 1, :]
            a = jnp.exp(jnp.minimum(later[:half] - earlier[:, :half], 0.0))
            a = (top * a * dt[:, :half]).astype(bf16)
            b = jnp.exp(jnp.minimum(later[half:] - earlier, 0.0))
            b = (low * b * dt).astype(bf16)
            ya = jnp.dot(a, xt[:half], preferred_element_type=f32)
            yb = jnp.dot(b, xt, preferred_element_type=f32)
            if k == 0:
                up, down = ya, yb
            else:
                up = jnp.where(lane >= k * head_size, ya, up)
                down = jnp.where(lane >= k * head_size, yb, down)
        skip = skip_ref[:, at] * xt.astype(f32)
        y_ref[:half, at] = up + skip[:half]
        y_ref[half:, at] = down + skip[half:]


def carry_kernel(got_ref, out_ref):
    count, rows, width = out_ref.shape
    carried = jnp.zeros((rows, width), f32)
    for k in range(count):
        out_ref[k] = carried.astype(bf16)
        both = got_ref[k].astype(f32)
        decay = both[rows : rows + 1] + both[rows + 1 : rows + 2]
        carried = decay * carried + both[:rows]


def gated_kernel(head_size, y_ref, bc_ref, cum_ref, ls_ref, pdec_ref, carried_ref, gate_ref, gain_ref, g_ref, ss_ref):
    width = y_ref.shape[1]
    n = bc_ref.shape[1] // 2
    entering = (ls_ref[0] + pdec_ref[0, 0:1] * carried_ref[...].astype(f32)).astype(bf16)
    cross = jnp.dot(bc_ref[:, n:], entering, preferred_element_type=f32)
    decay = jnp.exp(cum_ref[...])
    lane = lax.broadcasted_iota(jnp.int32, (1, LANES), 1)
    total = jnp.zeros((y_ref.shape[0], LANES), f32)
    for j in range(width // LANES):
        at = slice(j * LANES, (j + 1) * LANES)
        y = y_ref[:, at] + spread(decay, j, head_size, lane) * cross[:, at]
        gated = y * half_silu(gate_ref[:, at].astype(f32))
        total = total + gated * gated
        g_ref[:, at] = (gated * gain_ref[:, at]).astype(bf16)
    ss_ref[...] = jnp.broadcast_to(jnp.sum(total, axis=1, keepdims=True), ss_ref.shape)


def on_device(
    tokens,
    pre_gain,
    inner_proj,
    outer_proj,
    kernel_x,
    kernel_bc,
    offset_x,
    offset_bc,
    dt_bias,
    a_log,
    skip_gain,
    norm_gain,
    out_proj,
):
    width = inner_proj.shape[2]
    heads = dt_bias.shape[0]
    head_size = width // heads
    n = kernel_bc.shape[1] // 2
    rows_own = tokens.shape[0]
    group = lax.axis_size("head")
    line = lax.axis_size("seq")
    rows = rows_own * group
    blocks = rows // SPAN
    me = lax.axis_index("head")

    w_gate = inner_proj[:, 0, :]
    w_x = inner_proj[:, 1, :]
    w_dt = lax.dynamic_slice_in_dim(outer_proj[:, 2 * n :], me * heads, heads, 1)
    w_outer = jnp.concatenate([outer_proj[:, : 2 * n], jnp.pad(w_dt, ((0, 0), (0, LANES - heads)))], axis=1)

    parts = {0: row_norm(tokens, pre_gain).astype(bf16)}
    distance = group // 2
    while distance:
        for k in list(parts):
            parts[k ^ distance] = swapped(parts[k], "head", distance)
        distance //= 2
    normed = jnp.zeros((rows, tokens.shape[1]), bf16)
    for k in parts:
        normed = lax.dynamic_update_slice_in_dim(normed, parts[k], (me ^ k) * rows_own, 0)

    x_in = jnp.dot(normed, w_x, preferred_element_type=f32).astype(bf16)
    outer = jnp.dot(normed, w_outer, preferred_element_type=f32)
    bc_in = outer[:, : 2 * n].astype(bf16)
    tail = jnp.concatenate([x_in[rows - HALO :], bc_in[rows - HALO :]], axis=1)
    tail = lax.ppermute(tail, "seq", [(i, i + 1) for i in range(line - 1)])
    gate_in = jnp.dot(normed, w_gate, preferred_element_type=f32).astype(bf16)

    pad = (0, LANES - heads)
    dt = jax.nn.softplus(outer[:, 2 * n :] + jnp.pad(dt_bias, pad))
    rate = jnp.pad(-jnp.exp(a_log), pad)[None]

    def blocked(*shape):
        return pl.BlockSpec(shape, lambda i: (i,) + (0,) * (len(shape) - 1))

    def whole(*shape):
        return pl.BlockSpec(shape, lambda i: (0,) * len(shape))

    params = pltpu.CompilerParams(dimension_semantics=("arbitrary",), vmem_limit_bytes=40 << 20)
    shape = jax.ShapeDtypeStruct
    taps = kernel_x.shape[0]
    xc, bc, cum, cum_t, dt_t, local_state, prefix_decay, summary, decay = pl.pallas_call(
        lambda *refs: state_kernel(head_size, *refs),
        grid=(blocks,),
        in_specs=[
            blocked(SPAN, width), blocked(SPAN, 2 * n), whole(HALO, width), whole(HALO, 2 * n), blocked(SPAN, LANES),
            whole(1, LANES), whole(taps, width), whole(taps, 2 * n), whole(1, width), whole(1, 2 * n),
        ],
        out_specs=[
            blocked(SPAN, width), blocked(SPAN, 2 * n), blocked(SPAN, LANES), blocked(1, LANES, SPAN),
            blocked(1, LANES, SPAN), blocked(1, n, width), blocked(1, 8, width), whole(n, width), whole(8, width),
        ],
        out_shape=[
            shape((rows, width), bf16), shape((rows, 2 * n), bf16), shape((rows, LANES), f32),
            shape((blocks, LANES, SPAN), f32), shape((blocks, LANES, SPAN), f32), shape((blocks, n, width), f32),
            shape((blocks, 8, width), f32), shape((n, width), bf16), shape((8, width), bf16),
        ],
        scratch_shapes=[
            pltpu.VMEM((HALO, width), bf16), pltpu.VMEM((HALO, 2 * n), bf16), pltpu.VMEM((n, width), f32),
            pltpu.VMEM((8, width), f32), pltpu.VMEM((SPAN, width), bf16),
        ],
        compiler_params=params,
        name="block_states",
    )(x_in, bc_in, tail[:, :width], tail[:, width:], dt, rate, kernel_x, kernel_bc, offset_x[None], offset_bc[None])

    own = n // line
    sent = jnp.concatenate(
        [summary.reshape(line, own, width), jnp.broadcast_to(decay[None], (line, 8, width))], axis=1
    )
    got = lax.all_to_all(sent, "seq", 0, 0, tiled=True)
    carries = pl.pallas_call(carry_kernel, out_shape=shape((line, own, width), bf16), name="carries")(got)
    carried = lax.all_to_all(carries, "seq", 0, 0, tiled=True).reshape(n, width)

    y = pl.pallas_call(
        lambda *refs: inside_kernel(head_size, *refs),
        grid=(blocks,),
        in_specs=[
            blocked(SPAN, width), blocked(SPAN, 2 * n), blocked(SPAN, LANES), blocked(1, LANES, SPAN),
            blocked(1, LANES, SPAN), whole(1, width),
        ],
        out_specs=blocked(SPAN, width),
        out_shape=shape((rows, width), f32),
        compiler_params=params,
        name="inside_blocks",
    )(xc, bc, cum, cum_t, dt_t, jnp.repeat(skip_gain, head_size)[None])

    g, squares = pl.pallas_call(
        lambda *refs: gated_kernel(head_size, *refs),
        grid=(blocks,),
        in_specs=[
            blocked(SPAN, width), blocked(SPAN, 2 * n), blocked(SPAN, LANES), blocked(1, n, width),
            blocked(1, 8, width), whole(n, width), blocked(SPAN, width), whole(1, width),
        ],
        out_specs=[blocked(SPAN, width), blocked(SPAN, LANES)],
        out_shape=[shape((rows, width), bf16), shape((rows, LANES), f32)],
        compiler_params=params,
        name="gated",
    )(y, bc, cum, local_state, prefix_decay, carried, gate_in, norm_gain[None])

    squares = squares[:, 0]
    distance = 1
    while distance < group:
        squares = squares + swapped(squares, "head", distance)
        distance *= 2
    mine = lax.dynamic_slice_in_dim(squares, me * rows_own, rows_own, 0)
    inverse_rms = lax.rsqrt(mine / (width * group) + norm_floor)

    half = rows // 2
    top_bit = group // 2
    far = lax.dynamic_slice_in_dim(g, ((me ^ top_bit) // top_bit) * half, half, 0)
    near = lax.dynamic_slice_in_dim(g, (me // top_bit) * half, half, 0)
    far = jnp.dot(far, out_proj, preferred_element_type=f32).astype(bf16)
    near = jnp.dot(near, out_proj, preferred_element_type=f32).astype(bf16)
    parts = {}
    for k in range(group):
        source = far if k & top_bit else near
        parts[k] = lax.dynamic_slice_in_dim(source, ((me ^ k) % top_bit) * rows_own, rows_own, 0)
    distance = 1
    while distance < group:
        for k in reversed([k for k in parts if k & distance]):
            arrived = swapped(parts.pop(k), "head", distance)
            parts[k ^ distance] = parts[k ^ distance].astype(f32) + arrived.astype(f32)
            if distance * 2 < group:
                parts[k ^ distance] = parts[k ^ distance].astype(bf16)
        distance *= 2
    return (parts[0] * inverse_rms[:, None]).astype(bf16)


def solution(mesh):
    return jax.shard_map(
        on_device,
        mesh=mesh,
        in_specs=(
            P(("seq", "head"), None),
            P(),
            P(None, None, "head"),
            P(),
            P(None, "head"),
            P(),
            P("head"),
            P(),
            P("head"),
            P("head"),
            P("head"),
            P("head"),
            P("head", None),
        ),
        out_specs=P(("seq", "head"), None),
        check_vma=False,
    )
```

```python
import jax
import jax.numpy as jnp
from jax import lax
from jax.experimental import pallas as pl
from jax.experimental.pallas import tpu as pltpu
from jax.sharding import PartitionSpec as P

SPAN = 256
LANES = 128
HALO = 16

norm_floor = 0.1
bf16 = jnp.bfloat16
f32 = jnp.float32


def swapped(block, axis, distance):
    return lax.ppermute(block, axis, [(i, i ^ distance) for i in range(lax.axis_size(axis))])


def row_norm(row_block, gain_vector):
    widened = row_block.astype(f32)
    inverse_rms = lax.rsqrt(jnp.mean(widened * widened, axis=-1, keepdims=True) + norm_floor)
    return widened * inverse_rms * gain_vector


def half_silu(u):
    v = 0.5 * u
    return v + v * jnp.tanh(v)


def spread(per_head, tile, head_size, lane):
    per_tile = LANES // head_size
    first = tile * per_tile
    out = per_head[:, first : first + 1]
    for k in range(1, per_tile):
        out = jnp.where(lane >= k * head_size, per_head[:, first + k : first + k + 1], out)
    return out


def conv_tile(now, before, taps, bias):
    rows = now.shape[0]
    stacked = jnp.concatenate([before.astype(f32)[HALO - 8 :], now.astype(f32)], axis=0)
    count = taps.shape[0]
    total = bias + taps[count - 1 : count] * stacked[8:]
    for k in range(count - 1):
        moved = pltpu.roll(stacked, count - 1 - k, 0)[8:]
        total = total + taps[k : k + 1] * moved
    return half_silu(total).astype(bf16)


def in_place(at_ref, whole_ref, near_ref, far_ref):
    half = near_ref.shape[0]
    at = pl.multiple_of(at_ref[0], HALO)
    whole_ref[pl.ds(at, half), :] = near_ref[...]
    whole_ref[pl.ds(pl.multiple_of(half - at, HALO), half), :] = far_ref[...]


def state_kernel(head_size, at_ref, near_ref, far_ref, bc_ref, tail_x_ref, tail_bc_ref, dt_ref, rate_ref, kx_ref, kbc_ref, ox_ref, obc_ref,
                 xc_ref, bco_ref, cum_ref, cumt_ref, dtt_ref, ls_ref, pdec_ref, sum_ref, dec_ref,
                 px, pbc, state, logs, xw, x_all):
    step = pl.program_id(0)
    span, width = xc_ref.shape
    n = bc_ref.shape[1] // 2

    @pl.when(step == 0)
    def _():
        px[...] = tail_x_ref[...]
        pbc[...] = tail_bc_ref[...]
        state[...] = jnp.zeros_like(state)
        logs[...] = jnp.zeros_like(logs)
        in_place(at_ref, x_all, near_ref, far_ref)

    x_ref = x_all.at[pl.ds(pl.multiple_of(step * span, span), span), :]
    for j in range(2 * n // LANES):
        at = slice(j * LANES, (j + 1) * LANES)
        bco_ref[:, at] = conv_tile(bc_ref[:, at], pbc[:, at], kbc_ref[:, at], obc_ref[:, at])
    row = lax.broadcasted_iota(jnp.int32, (span, span), 0)
    col = lax.broadcasted_iota(jnp.int32, (span, span), 1)
    lower = (row >= col).astype(f32)
    dt = dt_ref[...]
    cum = jnp.dot(lower, dt * rate_ref[...], precision=lax.Precision.HIGHEST, preferred_element_type=f32)
    cum_ref[...] = cum
    cumt_ref[0] = cum.T
    dtt_ref[0] = dt.T
    end = cum[span - 1 :]
    weight = jnp.exp(end - cum) * dt
    ls_ref[0] = state[...]
    pdec_ref[0] = jnp.exp(logs[...])
    lane = lax.broadcasted_iota(jnp.int32, (1, LANES), 1)
    for j in range(width // LANES):
        at = slice(j * LANES, (j + 1) * LANES)
        xb = conv_tile(x_ref[:, at], px[:, at], kx_ref[:, at], ox_ref[:, at])
        xc_ref[:, at] = xb
        xw[:, at] = (xb.astype(f32) * spread(weight, j, head_size, lane)).astype(bf16)
        end_tile = spread(end, j, head_size, lane)
        logs[:, at] = logs[:, at] + end_tile
        state[:, at] = state[:, at] * jnp.exp(end_tile)
    state[...] = state[...] + lax.dot_general(
        bco_ref[:, :n], xw[...], (((0,), (0,)), ((), ())), preferred_element_type=f32
    )
    px[...] = x_ref[span - HALO :, :]
    pbc[...] = bc_ref[span - HALO :, :]

    @pl.when(step == pl.num_programs(0) - 1)
    def _():
        sum_ref[...] = state[...].astype(bf16)
        total = jnp.exp(logs[...])
        high = total.astype(bf16).astype(f32)
        which = lax.broadcasted_iota(jnp.int32, total.shape, 0)
        dec_ref[...] = jnp.where(which == 0, high, jnp.where(which == 1, total - high, 0.0)).astype(bf16)


def inside_kernel(head_size, x_ref, bc_ref, cum_ref, cumt_ref, dtt_ref, skip_ref, y_ref):
    span, width = x_ref.shape
    n = bc_ref.shape[1] // 2
    half = span // 2
    score = lax.dot_general(
        bc_ref[:, n:], bc_ref[:, :n], (((1,), (1,)), ((), ())), preferred_element_type=f32
    )
    row = lax.broadcasted_iota(jnp.int32, (span, span), 0)
    col = lax.broadcasted_iota(jnp.int32, (span, span), 1)
    score = jnp.where(row >= col, score, 0.0)
    top = score[:half, :half]
    low = score[half:]
    per_tile = LANES // head_size
    lane = lax.broadcasted_iota(jnp.int32, (1, LANES), 1)
    for j in range(width // LANES):
        at = slice(j * LANES, (j + 1) * LANES)
        xt = x_ref[:, at]
        up = down = None
        for k in range(per_tile):
            h = j * per_tile + k
            later = cum_ref[:, h : h + 1]
            earlier = cumt_ref[0, h : h + 1, :]
            dt = dtt_ref[0, h : h + 1, :]
            a = jnp.exp(jnp.minimum(later[:half] - earlier[:, :half], 0.0))
            a = (top * a * dt[:, :half]).astype(bf16)
            b = jnp.exp(jnp.minimum(later[half:] - earlier, 0.0))
            b = (low * b * dt).astype(bf16)
            ya = jnp.dot(a, xt[:half], preferred_element_type=f32)
            yb = jnp.dot(b, xt, preferred_element_type=f32)
            if k == 0:
                up, down = ya, yb
            else:
                up = jnp.where(lane >= k * head_size, ya, up)
                down = jnp.where(lane >= k * head_size, yb, down)
        skip = skip_ref[:, at] * xt.astype(f32)
        y_ref[:half, at] = (up + skip[:half]).astype(bf16)
        y_ref[half:, at] = (down + skip[half:]).astype(bf16)


def carry_kernel(got_ref, out_ref):
    count, rows, width = out_ref.shape
    carried = jnp.zeros((rows, width), f32)
    for k in range(count):
        out_ref[k] = carried.astype(bf16)
        both = got_ref[k].astype(f32)
        decay = both[rows : rows + 1] + both[rows + 1 : rows + 2]
        carried = decay * carried + both[:rows]


def gated_kernel(head_size, y_ref, bc_ref, cum_ref, ls_ref, pdec_ref, carried_ref, at_ref, near_ref, far_ref, gain_ref,
                 g_ref, ss_ref, gate_all):
    span, width = y_ref.shape
    step = pl.program_id(0)

    @pl.when(step == 0)
    def _():
        in_place(at_ref, gate_all, near_ref, far_ref)

    gate_ref = gate_all.at[pl.ds(pl.multiple_of(step * span, span), span), :]
    n = bc_ref.shape[1] // 2
    entering = (ls_ref[0] + pdec_ref[0, 0:1] * carried_ref[...].astype(f32)).astype(bf16)
    cross = jnp.dot(bc_ref[:, n:], entering, preferred_element_type=f32)
    decay = jnp.exp(cum_ref[...])
    lane = lax.broadcasted_iota(jnp.int32, (1, LANES), 1)
    total = jnp.zeros((y_ref.shape[0], LANES), f32)
    for j in range(width // LANES):
        at = slice(j * LANES, (j + 1) * LANES)
        y = y_ref[:, at].astype(f32) + spread(decay, j, head_size, lane) * cross[:, at]
        gated = y * half_silu(gate_ref[:, at].astype(f32))
        total = total + gated * gated
        g_ref[:, at] = (gated * gain_ref[:, at]).astype(bf16)
    ss_ref[...] = jnp.broadcast_to(jnp.sum(total, axis=1, keepdims=True), ss_ref.shape)


def on_device(
    tokens,
    pre_gain,
    inner_proj,
    outer_proj,
    kernel_x,
    kernel_bc,
    offset_x,
    offset_bc,
    dt_bias,
    a_log,
    skip_gain,
    norm_gain,
    out_proj,
):
    width = inner_proj.shape[2]
    heads = dt_bias.shape[0]
    head_size = width // heads
    n = kernel_bc.shape[1] // 2
    rows_own = tokens.shape[0]
    group = lax.axis_size("head")
    line = lax.axis_size("seq")
    rows = rows_own * group
    blocks = rows // SPAN
    me = lax.axis_index("head")

    joined = inner_proj.reshape(inner_proj.shape[0], 2 * width)
    w_gate, w_x = joined[:, :width], joined[:, width:]
    w_dt = lax.dynamic_slice_in_dim(outer_proj[:, 2 * n :], me * heads, heads, 1)
    w_outer = jnp.concatenate([outer_proj[:, : 2 * n], jnp.pad(w_dt, ((0, 0), (0, LANES - heads)))], axis=1)

    top_bit = group // 2
    half = rows // 2
    upper = me >= top_bit
    near = row_norm(tokens, pre_gain).astype(bf16)
    far = swapped(near, "head", top_bit)

    def gathered(block):
        distance = 1
        while distance < top_bit:
            other = swapped(block, "head", distance)
            last = (me & distance) > 0
            block = jnp.where(
                last, jnp.concatenate([other, block], axis=0), jnp.concatenate([block, other], axis=0)
            )
            distance *= 2
        return block

    def projected(block):
        x_part = jnp.dot(block, w_x, preferred_element_type=f32).astype(bf16)
        outer_part = jnp.dot(block, w_outer, preferred_element_type=f32)
        gate_part = jnp.dot(block, w_gate, preferred_element_type=f32).astype(bf16)
        return x_part, outer_part, gate_part

    def ordered(near_part, far_part):
        return jnp.where(
            upper,
            jnp.concatenate([far_part, near_part], axis=0),
            jnp.concatenate([near_part, far_part], axis=0),
        )

    x_near, outer_near, gate_near = projected(gathered(near))
    far, x_near, outer_near, gate_near = lax.optimization_barrier((far, x_near, outer_near, gate_near))
    x_far, outer_far, gate_far = projected(gathered(far))
    outer = ordered(outer_near, outer_far)
    bc_in = outer[:, : 2 * n].astype(bf16)
    x_end = jnp.where(upper, x_near[half - HALO :], x_far[half - HALO :])
    tail = jnp.concatenate([x_end, bc_in[rows - HALO :]], axis=1)
    tail = lax.ppermute(tail, "seq", [(i, i + 1) for i in range(line - 1)])
    near_at = jnp.where(upper, half, 0).astype(jnp.int32).reshape(1)

    pad = (0, LANES - heads)
    dt = jax.nn.softplus(outer[:, 2 * n :] + jnp.pad(dt_bias, pad))
    rate = jnp.pad(-jnp.exp(a_log), pad)[None]

    def blocked(*shape):
        return pl.BlockSpec(shape, lambda i: (i,) + (0,) * (len(shape) - 1))

    def whole(*shape):
        return pl.BlockSpec(shape, lambda i: (0,) * len(shape))

    def params(mib):
        return pltpu.CompilerParams(dimension_semantics=("arbitrary",), vmem_limit_bytes=mib << 20)

    scalar = pl.BlockSpec(memory_space=pltpu.SMEM)
    shape = jax.ShapeDtypeStruct
    taps = kernel_x.shape[0]
    xc, bc, cum, cum_t, dt_t, local_state, prefix_decay, summary, decay = pl.pallas_call(
        lambda *refs: state_kernel(head_size, *refs),
        grid=(blocks,),
        in_specs=[
            scalar, whole(half, width), whole(half, width), blocked(SPAN, 2 * n), whole(HALO, width), whole(HALO, 2 * n), blocked(SPAN, LANES),
            whole(1, LANES), whole(taps, width), whole(taps, 2 * n), whole(1, width), whole(1, 2 * n),
        ],
        out_specs=[
            blocked(SPAN, width), blocked(SPAN, 2 * n), blocked(SPAN, LANES), blocked(1, LANES, SPAN),
            blocked(1, LANES, SPAN), blocked(1, n, width), blocked(1, 8, width), whole(n, width), whole(8, width),
        ],
        out_shape=[
            shape((rows, width), bf16), shape((rows, 2 * n), bf16), shape((rows, LANES), f32),
            shape((blocks, LANES, SPAN), f32), shape((blocks, LANES, SPAN), f32), shape((blocks, n, width), f32),
            shape((blocks, 8, width), f32), shape((n, width), bf16), shape((8, width), bf16),
        ],
        scratch_shapes=[
            pltpu.VMEM((HALO, width), bf16), pltpu.VMEM((HALO, 2 * n), bf16), pltpu.VMEM((n, width), f32),
            pltpu.VMEM((8, width), f32), pltpu.VMEM((SPAN, width), bf16), pltpu.VMEM((rows, width), bf16),
        ],
        compiler_params=params(24),
        name="block_states",
    )(near_at, x_near, x_far, bc_in, tail[:, :width], tail[:, width:], dt, rate, kernel_x, kernel_bc, offset_x[None], offset_bc[None])

    own = n // line
    sent = jnp.concatenate(
        [summary.reshape(line, own, width), jnp.broadcast_to(decay[None], (line, 8, width))], axis=1
    )
    got = lax.all_to_all(sent, "seq", 0, 0, tiled=True)
    y = pl.pallas_call(
        lambda *refs: inside_kernel(head_size, *refs),
        grid=(blocks,),
        in_specs=[
            blocked(SPAN, width), blocked(SPAN, 2 * n), blocked(SPAN, LANES), blocked(1, LANES, SPAN),
            blocked(1, LANES, SPAN), whole(1, width),
        ],
        out_specs=blocked(SPAN, width),
        out_shape=shape((rows, width), bf16),
        compiler_params=params(12),
        cost_estimate=pl.CostEstimate(flops=8 * rows * SPAN * width, transcendentals=0, bytes_accessed=0),
        name="inside_blocks",
    )(xc, bc, cum, cum_t, dt_t, jnp.repeat(skip_gain, head_size)[None])

    got, y = lax.optimization_barrier((got, y))
    carries = pl.pallas_call(
        carry_kernel,
        out_shape=shape((line, own, width), bf16),
        compiler_params=pltpu.CompilerParams(vmem_limit_bytes=8 << 20),
        name="carries",
    )(got)
    carried = lax.all_to_all(carries, "seq", 0, 0, tiled=True).reshape(n, width)

    g, squares = pl.pallas_call(
        lambda *refs: gated_kernel(head_size, *refs),
        grid=(blocks,),
        in_specs=[
            blocked(SPAN, width), blocked(SPAN, 2 * n), blocked(SPAN, LANES), blocked(1, n, width),
            blocked(1, 8, width), whole(n, width), scalar, whole(half, width), whole(half, width), whole(1, width),
        ],
        out_specs=[blocked(SPAN, width), blocked(SPAN, LANES)],
        out_shape=[shape((rows, width), bf16), shape((rows, LANES), f32)],
        scratch_shapes=[pltpu.VMEM((rows, width), bf16)],
        compiler_params=params(20),
        name="gated",
    )(y, bc, cum, local_state, prefix_decay, carried, near_at, gate_near, gate_far, norm_gain[None])

    squares = squares[:, 0]
    distance = 1
    while distance < group:
        squares = squares + swapped(squares, "head", distance)
        distance *= 2
    mine = lax.dynamic_slice_in_dim(squares, me * rows_own, rows_own, 0)
    inverse_rms = lax.rsqrt(mine / (width * group) + norm_floor)

    parts = {}
    for k in reversed(range(group)):
        own_rows = lax.dynamic_slice_in_dim(g, (me ^ k) * rows_own, rows_own, 0)
        parts[k] = lax.optimization_barrier(jnp.dot(own_rows, out_proj, preferred_element_type=f32).astype(bf16))
    distance = 1
    while distance < group:
        for k in sorted((k for k in parts if k & distance), reverse=True):
            arrived = swapped(parts.pop(k), "head", distance)
            parts[k ^ distance] = parts[k ^ distance].astype(f32) + arrived.astype(f32)
            if distance * 2 < group:
                parts[k ^ distance] = parts[k ^ distance].astype(bf16)
        distance *= 2
    return (parts[0] * inverse_rms[:, None]).astype(bf16)


def solution(mesh):
    return jax.shard_map(
        on_device,
        mesh=mesh,
        in_specs=(
            P(("seq", "head"), None),
            P(),
            P(None, None, "head"),
            P(),
            P(None, "head"),
            P(),
            P("head"),
            P(),
            P("head"),
            P("head"),
            P("head"),
            P("head"),
            P("head", None),
        ),
        out_specs=P(("seq", "head"), None),
        check_vma=False,
    )
```

```python
import jax
import jax.numpy as jnp
from jax import lax
from jax.experimental import pallas as pl
from jax.experimental.pallas import tpu as pltpu
from jax.sharding import PartitionSpec as P

SPAN = 256
LANES = 128
HALO = 16

norm_floor = 0.1
bf16 = jnp.bfloat16
f32 = jnp.float32


def swapped(block, axis, distance):
    return lax.ppermute(block, axis, [(i, i ^ distance) for i in range(lax.axis_size(axis))])


def row_norm(row_block, gain_vector):
    widened = row_block.astype(f32)
    inverse_rms = lax.rsqrt(jnp.mean(widened * widened, axis=-1, keepdims=True) + norm_floor)
    return widened * inverse_rms * gain_vector


def half_silu(u):
    v = 0.5 * u
    return v + v * jnp.tanh(v)


def spread(per_head, tile, head_size, lane):
    per_tile = LANES // head_size
    first = tile * per_tile
    out = per_head[:, first : first + 1]
    for k in range(1, per_tile):
        out = jnp.where(lane >= k * head_size, per_head[:, first + k : first + k + 1], out)
    return out


def conv_tile(now, before, taps, bias):
    rows = now.shape[0]
    stacked = jnp.concatenate([before.astype(f32)[HALO - 8 :], now.astype(f32)], axis=0)
    count = taps.shape[0]
    total = bias + taps[count - 1 : count] * stacked[8:]
    for k in range(count - 1):
        moved = pltpu.roll(stacked, count - 1 - k, 0)[8:]
        total = total + taps[k : k + 1] * moved
    return half_silu(total).astype(bf16)


def in_place(at_ref, whole_ref, near_ref, far_ref):
    half = near_ref.shape[0]
    at = pl.multiple_of(at_ref[0], HALO)
    whole_ref[pl.ds(at, half), :] = near_ref[...]
    whole_ref[pl.ds(pl.multiple_of(half - at, HALO), half), :] = far_ref[...]


def state_kernel(head_size, at_ref, near_ref, far_ref, bc_ref, tail_x_ref, tail_bc_ref, dt_ref, rate_ref, kx_ref, kbc_ref, ox_ref, obc_ref,
                 xc_ref, bco_ref, cum_ref, cumt_ref, dtt_ref, ls_ref, pdec_ref, sum_ref, dec_ref,
                 px, pbc, state, logs, xw, x_all):
    step = pl.program_id(0)
    span, width = xc_ref.shape
    n = bc_ref.shape[1] // 2

    @pl.when(step == 0)
    def _():
        px[...] = tail_x_ref[...]
        pbc[...] = tail_bc_ref[...]
        state[...] = jnp.zeros_like(state)
        logs[...] = jnp.zeros_like(logs)
        in_place(at_ref, x_all, near_ref, far_ref)

    x_ref = x_all.at[pl.ds(pl.multiple_of(step * span, span), span), :]
    for j in range(2 * n // LANES):
        at = slice(j * LANES, (j + 1) * LANES)
        bco_ref[:, at] = conv_tile(bc_ref[:, at], pbc[:, at], kbc_ref[:, at], obc_ref[:, at])
    row = lax.broadcasted_iota(jnp.int32, (span, span), 0)
    col = lax.broadcasted_iota(jnp.int32, (span, span), 1)
    lower = (row >= col).astype(f32)
    dt = dt_ref[...]
    cum = jnp.dot(lower, dt * rate_ref[...], precision=lax.Precision.HIGHEST, preferred_element_type=f32)
    cum_ref[...] = cum
    cumt_ref[0] = cum.T
    dtt_ref[0] = dt.T
    end = cum[span - 1 :]
    weight = jnp.exp(end - cum) * dt
    ls_ref[0] = state[...]
    pdec_ref[0] = jnp.exp(logs[...])
    lane = lax.broadcasted_iota(jnp.int32, (1, LANES), 1)
    for j in range(width // LANES):
        at = slice(j * LANES, (j + 1) * LANES)
        xb = conv_tile(x_ref[:, at], px[:, at], kx_ref[:, at], ox_ref[:, at])
        xc_ref[:, at] = xb
        xw[:, at] = (xb.astype(f32) * spread(weight, j, head_size, lane)).astype(bf16)
        end_tile = spread(end, j, head_size, lane)
        logs[:, at] = logs[:, at] + end_tile
        state[:, at] = state[:, at] * jnp.exp(end_tile)
    state[...] = state[...] + lax.dot_general(
        bco_ref[:, :n], xw[...], (((0,), (0,)), ((), ())), preferred_element_type=f32
    )
    px[...] = x_ref[span - HALO :, :]
    pbc[...] = bc_ref[span - HALO :, :]

    @pl.when(step == pl.num_programs(0) - 1)
    def _():
        sum_ref[...] = state[...].astype(bf16)
        total = jnp.exp(logs[...])
        high = total.astype(bf16).astype(f32)
        which = lax.broadcasted_iota(jnp.int32, total.shape, 0)
        dec_ref[...] = jnp.where(which == 0, high, jnp.where(which == 1, total - high, 0.0)).astype(bf16)


def inside_kernel(head_size, x_ref, bc_ref, cum_ref, cumt_ref, dtt_ref, skip_ref, y_ref):
    span, width = x_ref.shape
    n = bc_ref.shape[1] // 2
    half = span // 2
    score = lax.dot_general(
        bc_ref[:, n:], bc_ref[:, :n], (((1,), (1,)), ((), ())), preferred_element_type=f32
    )
    row = lax.broadcasted_iota(jnp.int32, (span, span), 0)
    col = lax.broadcasted_iota(jnp.int32, (span, span), 1)
    score = jnp.where(row >= col, score, 0.0)
    top = score[:half, :half]
    low = score[half:]
    per_tile = LANES // head_size
    lane = lax.broadcasted_iota(jnp.int32, (1, LANES), 1)
    for j in range(width // LANES):
        at = slice(j * LANES, (j + 1) * LANES)
        xt = x_ref[:, at]
        up = down = None
        for k in range(per_tile):
            h = j * per_tile + k
            later = cum_ref[:, h : h + 1]
            earlier = cumt_ref[0, h : h + 1, :]
            dt = dtt_ref[0, h : h + 1, :]
            a = jnp.exp(jnp.minimum(later[:half] - earlier[:, :half], 0.0))
            a = (top * a * dt[:, :half]).astype(bf16)
            b = jnp.exp(jnp.minimum(later[half:] - earlier, 0.0))
            b = (low * b * dt).astype(bf16)
            ya = jnp.dot(a, xt[:half], preferred_element_type=f32)
            yb = jnp.dot(b, xt, preferred_element_type=f32)
            if k == 0:
                up, down = ya, yb
            else:
                up = jnp.where(lane >= k * head_size, ya, up)
                down = jnp.where(lane >= k * head_size, yb, down)
        skip = skip_ref[:, at] * xt.astype(f32)
        y_ref[:half, at] = (up + skip[:half]).astype(bf16)
        y_ref[half:, at] = (down + skip[half:]).astype(bf16)


def carry_kernel(got_ref, out_ref):
    count, rows, width = out_ref.shape
    carried = jnp.zeros((rows, width), f32)
    for k in range(count):
        out_ref[k] = carried.astype(bf16)
        both = got_ref[k].astype(f32)
        decay = both[rows : rows + 1] + both[rows + 1 : rows + 2]
        carried = decay * carried + both[:rows]


def gated_kernel(head_size, y_ref, bc_ref, cum_ref, ls_ref, pdec_ref, carried_ref, at_ref, near_ref, far_ref, gain_ref,
                 g_ref, ss_ref, gate_all):
    span, width = y_ref.shape
    step = pl.program_id(0)

    @pl.when(step == 0)
    def _():
        in_place(at_ref, gate_all, near_ref, far_ref)

    gate_ref = gate_all.at[pl.ds(pl.multiple_of(step * span, span), span), :]
    n = bc_ref.shape[1] // 2
    entering = (ls_ref[0] + pdec_ref[0, 0:1] * carried_ref[...].astype(f32)).astype(bf16)
    cross = jnp.dot(bc_ref[:, n:], entering, preferred_element_type=f32)
    decay = jnp.exp(cum_ref[...])
    lane = lax.broadcasted_iota(jnp.int32, (1, LANES), 1)
    total = jnp.zeros((y_ref.shape[0], LANES), f32)
    for j in range(width // LANES):
        at = slice(j * LANES, (j + 1) * LANES)
        y = y_ref[:, at].astype(f32) + spread(decay, j, head_size, lane) * cross[:, at]
        gated = y * half_silu(gate_ref[:, at].astype(f32))
        total = total + gated * gated
        g_ref[:, at] = (gated * gain_ref[:, at]).astype(bf16)
    ss_ref[...] = jnp.broadcast_to(jnp.sum(total, axis=1, keepdims=True), ss_ref.shape)


def on_device(
    tokens,
    pre_gain,
    inner_proj,
    outer_proj,
    kernel_x,
    kernel_bc,
    offset_x,
    offset_bc,
    dt_bias,
    a_log,
    skip_gain,
    norm_gain,
    out_proj,
):
    width = inner_proj.shape[2]
    heads = dt_bias.shape[0]
    head_size = width // heads
    n = kernel_bc.shape[1] // 2
    rows_own = tokens.shape[0]
    group = lax.axis_size("head")
    line = lax.axis_size("seq")
    rows = rows_own * group
    blocks = rows // SPAN
    me = lax.axis_index("head")

    joined = inner_proj.reshape(inner_proj.shape[0], 2 * width)
    w_gate, w_x = joined[:, :width], joined[:, width:]
    w_dt = lax.dynamic_slice_in_dim(outer_proj[:, 2 * n :], me * heads, heads, 1)
    w_outer = jnp.concatenate([outer_proj[:, : 2 * n], jnp.pad(w_dt, ((0, 0), (0, LANES - heads)))], axis=1)

    top_bit = group // 2
    half = rows // 2
    upper = me >= top_bit
    near = row_norm(tokens, pre_gain).astype(bf16)
    far = swapped(near, "head", top_bit)

    def gathered(block):
        distance = 1
        while distance < top_bit:
            other = swapped(block, "head", distance)
            last = (me & distance) > 0
            block = jnp.where(
                last, jnp.concatenate([other, block], axis=0), jnp.concatenate([block, other], axis=0)
            )
            distance *= 2
        return block

    def projected(block):
        x_part = jnp.dot(block, w_x, preferred_element_type=f32).astype(bf16)
        outer_part = jnp.dot(block, w_outer, preferred_element_type=f32)
        gate_part = jnp.dot(block, w_gate, preferred_element_type=f32).astype(bf16)
        return x_part, outer_part, gate_part

    def ordered(near_part, far_part):
        return jnp.where(
            upper,
            jnp.concatenate([far_part, near_part], axis=0),
            jnp.concatenate([near_part, far_part], axis=0),
        )

    x_near, outer_near, gate_near = projected(gathered(near))
    far, x_near, outer_near, gate_near = lax.optimization_barrier((far, x_near, outer_near, gate_near))
    x_far, outer_far, gate_far = projected(gathered(far))
    outer = ordered(outer_near, outer_far)
    bc_in = outer[:, : 2 * n].astype(bf16)
    x_end = jnp.where(upper, x_near[half - HALO :], x_far[half - HALO :])
    tail = jnp.concatenate([x_end, bc_in[rows - HALO :]], axis=1)
    tail = lax.ppermute(tail, "seq", [(i, i + 1) for i in range(line - 1)])
    near_at = jnp.where(upper, half, 0).astype(jnp.int32).reshape(1)

    pad = (0, LANES - heads)
    dt = jax.nn.softplus(outer[:, 2 * n :] + jnp.pad(dt_bias, pad))
    rate = jnp.pad(-jnp.exp(a_log), pad)[None]

    def blocked(*shape):
        return pl.BlockSpec(shape, lambda i: (i,) + (0,) * (len(shape) - 1))

    def whole(*shape):
        return pl.BlockSpec(shape, lambda i: (0,) * len(shape))

    def params(mib):
        return pltpu.CompilerParams(dimension_semantics=("arbitrary",), vmem_limit_bytes=mib << 20)

    scalar = pl.BlockSpec(memory_space=pltpu.SMEM)
    shape = jax.ShapeDtypeStruct
    taps = kernel_x.shape[0]
    xc, bc, cum, cum_t, dt_t, local_state, prefix_decay, summary, decay = pl.pallas_call(
        lambda *refs: state_kernel(head_size, *refs),
        grid=(blocks,),
        in_specs=[
            scalar, whole(half, width), whole(half, width), blocked(SPAN, 2 * n), whole(HALO, width), whole(HALO, 2 * n), blocked(SPAN, LANES),
            whole(1, LANES), whole(taps, width), whole(taps, 2 * n), whole(1, width), whole(1, 2 * n),
        ],
        out_specs=[
            blocked(SPAN, width), blocked(SPAN, 2 * n), blocked(SPAN, LANES), blocked(1, LANES, SPAN),
            blocked(1, LANES, SPAN), blocked(1, n, width), blocked(1, 8, width), whole(n, width), whole(8, width),
        ],
        out_shape=[
            shape((rows, width), bf16), shape((rows, 2 * n), bf16), shape((rows, LANES), f32),
            shape((blocks, LANES, SPAN), f32), shape((blocks, LANES, SPAN), f32), shape((blocks, n, width), f32),
            shape((blocks, 8, width), f32), shape((n, width), bf16), shape((8, width), bf16),
        ],
        scratch_shapes=[
            pltpu.VMEM((HALO, width), bf16), pltpu.VMEM((HALO, 2 * n), bf16), pltpu.VMEM((n, width), f32),
            pltpu.VMEM((8, width), f32), pltpu.VMEM((SPAN, width), bf16), pltpu.VMEM((rows, width), bf16),
        ],
        compiler_params=params(18),
        name="block_states",
    )(near_at, x_near, x_far, bc_in, tail[:, :width], tail[:, width:], dt, rate, kernel_x, kernel_bc, offset_x[None], offset_bc[None])

    own = n // line
    sent = jnp.concatenate(
        [summary.reshape(line, own, width), jnp.broadcast_to(decay[None], (line, 8, width))], axis=1
    )
    got = lax.all_to_all(sent, "seq", 0, 0, tiled=True)
    y = pl.pallas_call(
        lambda *refs: inside_kernel(head_size, *refs),
        grid=(blocks,),
        in_specs=[
            blocked(SPAN, width), blocked(SPAN, 2 * n), blocked(SPAN, LANES), blocked(1, LANES, SPAN),
            blocked(1, LANES, SPAN), whole(1, width),
        ],
        out_specs=blocked(SPAN, width),
        out_shape=shape((rows, width), bf16),
        compiler_params=params(12),
        cost_estimate=pl.CostEstimate(flops=8 * rows * SPAN * width, transcendentals=0, bytes_accessed=0),
        name="inside_blocks",
    )(xc, bc, cum, cum_t, dt_t, jnp.repeat(skip_gain, head_size)[None])

    got, y = lax.optimization_barrier((got, y))
    carries = pl.pallas_call(
        carry_kernel,
        out_shape=shape((line, own, width), bf16),
        compiler_params=pltpu.CompilerParams(vmem_limit_bytes=8 << 20),
        name="carries",
    )(got)
    carried = lax.all_to_all(carries, "seq", 0, 0, tiled=True).reshape(n, width)

    g, squares = pl.pallas_call(
        lambda *refs: gated_kernel(head_size, *refs),
        grid=(blocks,),
        in_specs=[
            blocked(SPAN, width), blocked(SPAN, 2 * n), blocked(SPAN, LANES), blocked(1, n, width),
            blocked(1, 8, width), whole(n, width), scalar, whole(half, width), whole(half, width), whole(1, width),
        ],
        out_specs=[blocked(SPAN, width), blocked(SPAN, LANES)],
        out_shape=[shape((rows, width), bf16), shape((rows, LANES), f32)],
        scratch_shapes=[pltpu.VMEM((rows, width), bf16)],
        compiler_params=params(14),
        name="gated",
    )(y, bc, cum, local_state, prefix_decay, carried, near_at, gate_near, gate_far, norm_gain[None])

    squares = squares[:, 0]
    distance = 1
    while distance < group:
        squares = squares + swapped(squares, "head", distance)
        distance *= 2
    mine = lax.dynamic_slice_in_dim(squares, me * rows_own, rows_own, 0)
    inverse_rms = lax.rsqrt(mine / (width * group) + norm_floor)

    far = lax.dynamic_slice_in_dim(g, jnp.where(upper, 0, half), half, 0)
    near = lax.dynamic_slice_in_dim(g, jnp.where(upper, half, 0), half, 0)
    far = jnp.dot(far, out_proj, preferred_element_type=f32).astype(bf16)
    near = jnp.dot(near, out_proj, preferred_element_type=f32).astype(bf16)
    parts = {}
    for k in range(group):
        source = far if k & top_bit else near
        parts[k] = lax.dynamic_slice_in_dim(source, ((me ^ k) % top_bit) * rows_own, rows_own, 0)
    distance = 1
    while distance < group:
        for k in sorted((k for k in parts if k & distance), reverse=True):
            arrived = swapped(parts.pop(k), "head", distance)
            parts[k ^ distance] = parts[k ^ distance].astype(f32) + arrived.astype(f32)
            if distance * 2 < group:
                parts[k ^ distance] = parts[k ^ distance].astype(bf16)
        distance *= 2
    return (parts[0] * inverse_rms[:, None]).astype(bf16)


def solution(mesh):
    return jax.shard_map(
        on_device,
        mesh=mesh,
        in_specs=(
            P(("seq", "head"), None),
            P(),
            P(None, None, "head"),
            P(),
            P(None, "head"),
            P(),
            P("head"),
            P(),
            P("head"),
            P("head"),
            P("head"),
            P("head"),
            P("head", None),
        ),
        out_specs=P(("seq", "head"), None),
        check_vma=False,
    )
```
